32 devices in a mesh: rows: 16 (over z, y, x), grp: 2 (over core).
Axes of the slice: x: 2, y: 2, z: 4, core: 2. Of those that a mesh axis runs over, the one named last changes fastest.
Arguments:
- perturb: bfloat16 [32768, 2040], P(('rows', 'grp')), may hold values from -6 to 6
- start_block: bfloat16 [2040, 128], replicated, may hold values from -6 to 6
Outputs:
- eofs: float32 [32768, 128], P(('rows', 'grp'))
- loadings: float32 [2040, 128], P('grp')
The draws below stay inside these ranges and needn't reach their ends.
All inputs are finite; a program needn't handle non-finite values.
Results may differ from the reference program's by a relative error of at most 0.009.
Values may be sent and summed in bfloat16 or wider, within the bound.
A program may use at most 64 MiB of HBM per device.

```python
import math
import jax
import jax.numpy as jnp

COLS = 2040
RANK = 128
ITERS = 2
TOTAL_ROWS = 32768


def with_spikes(array, own_key, source, target, blocks, factor):
    def block_of(dim):
        return (jnp.arange(array.shape[dim]) // (array.shape[dim] // blocks)).reshape((-1,) + (1,) * (array.ndim - 1 - dim))

    one_side = jax.random.permutation(own_key, blocks)[block_of(target)]
    other_side = (block_of(target) + blocks // 2) % blocks
    return jnp.where((block_of(source) == one_side) | (block_of(source) == other_side), factor * array, array)


def steps_of(rng, shape, split, low, largest):
    level = 1.0
    for axis_at, parts in split:
        heights = jax.random.uniform(jax.random.fold_in(jax.random.fold_in(rng, 6), axis_at), (parts,), jnp.float32, low / len(split), largest / len(split))
        level = level * jnp.repeat(jnp.exp(heights), shape[axis_at] // parts).reshape((-1,) + (1,) * (len(shape) - 1 - axis_at))
    return level


def noise(rng, extent, scale, bound, shards=(), dtype=jnp.bfloat16):
    drawn = scale * jax.random.normal(rng, extent, jnp.float32)
    if shards:
        drawn = drawn * steps_of(rng, extent, shards, -0.22, 0.18)
    return jnp.clip(drawn, -bound, bound).astype(dtype)


def heavy_noise(rng, shape, scale, most, pieces, heavy, held_as=jnp.bfloat16):
    result = scale * jax.random.normal(rng, shape, jnp.float32)
    if pieces:
        result = result * steps_of(rng, shape, pieces, -0.22, 0.18)
    return jnp.clip(with_spikes(result, jax.random.fold_in(rng, 3), *heavy), -most, most).astype(held_as)


def setup_inputs(seed: int = 0) -> dict:
    arg_keys = jax.random.split(jax.random.key(seed), 3)
    perturb = heavy_noise(arg_keys[0], (TOTAL_ROWS, COLS), 1.0, 6.0, ((0, 32),), (0, 1, 8, 2.0))
    start_block = noise(arg_keys[1], (COLS, RANK), 1.0, 6.0)
    return dict(perturb=perturb, start_block=start_block)


def right_solve(factor, block):
    return jax.scipy.linalg.solve_triangular(factor, block.T, lower=True).T

def reference(perturb, start_block):
    basis_in = start_block
    for sweep in range(ITERS):
        projected = jnp.dot(perturb.astype(jnp.float32), basis_in.astype(jnp.float32), preferred_element_type=jnp.float32).astype(jnp.bfloat16)
        gram_sum = jnp.dot(projected.T.astype(jnp.float32), projected.astype(jnp.float32), preferred_element_type=jnp.float32)
        panel_sum = jnp.dot(perturb.T.astype(jnp.float32), projected.astype(jnp.float32), preferred_element_type=jnp.float32)
        factor = jnp.linalg.cholesky(gram_sum)
        weights = right_solve(factor, panel_sum)
        basis_in = weights.astype(jnp.bfloat16)
    eofs = right_solve(factor, projected.astype(jnp.float32)) * math.sqrt(TOTAL_ROWS)
    loadings = weights * math.sqrt(COLS / TOTAL_ROWS)
    return (eofs, loadings)
```

```python
import functools
import math

import jax
import jax.numpy as jnp
from jax import lax
from jax.experimental import pallas as pl
from jax.experimental.pallas import tpu as pltpu
from jax.sharding import PartitionSpec as P

ITERS = 2
LANES = 128
F32 = jnp.float32
BF16 = jnp.bfloat16
MESH = pl.DeviceIdType.MESH


def round_up(value, unit):
    return (value + unit - 1) // unit * unit


def each(start, stop, body):
    if stop - start <= 16:
        for index in range(start, stop):
            body(index)
    else:
        @pl.loop(start, stop)
        def _(index):
            body(index)


def nt_dot(a, b, **kw):
    return lax.dot_general(a, b, (((1,), (1,)), ((), ())), preferred_element_type=F32, **kw)


def tn_dot(a, b, **kw):
    return lax.dot_general(a, b, (((0,), (0,)), ((), ())), preferred_element_type=F32, **kw)


def inverse_factor(work, inverse):
    rank = inverse.shape[0]
    size = 8
    row = lax.broadcasted_iota(jnp.int32, (rank, rank), 0)
    column = lax.broadcasted_iota(jnp.int32, (rank, rank), 1)
    work[:, rank:] = (row == column).astype(F32)
    sublane = lax.broadcasted_iota(jnp.int32, (size, 2 * rank), 0)
    for at in range(0, rank, size):
        rows = work[at : at + size, :]
        columns = [
            jnp.broadcast_to(rows[:, at + k : at + k + 1], (size, rank)) for k in range(size)
        ]
        d = {
            (i, k): jnp.broadcast_to(columns[k][i : i + 1, :], (size, rank))
            for k in range(size)
            for i in range(k, size)
        }
        held = [
            [
                jnp.broadcast_to(rows[i : i + 1, h * rank : (h + 1) * rank], (size, rank))
                for h in range(2)
            ]
            for i in range(size)
        ]
        for k in range(size):
            scale = lax.rsqrt(d[k, k])
            held[k] = [part * scale for part in held[k]]
            low = {i: d[i, k] * scale for i in range(k + 1, size)}
            for j in range(k + 1, size):
                for i in range(j, size):
                    d[i, j] = d[i, j] - low[i] * low[j]
                held[j] = [held[j][h] - low[j] * held[k][h] for h in range(2)]
        block = jnp.concatenate(held[0], axis=1)
        for k in range(1, size):
            block = jnp.where(sublane == k, jnp.concatenate(held[k], axis=1), block)
        inverse[at : at + size, :] = block[:, rank:]
        if at + size < rank:
            first = block.astype(BF16).astype(F32)
            rest = block - first
            second = rest.astype(BF16).astype(F32)
            third = rest - second
            left = jnp.concatenate([first, first, second, first, third, second], axis=0)
            right = jnp.concatenate([first, second, first, third, first, second], axis=0)
            update = tn_dot(left[:, :rank].astype(BF16), right.astype(BF16))
            work[at + size :, :] = work[at + size :, :] - update[at + size :, :]


def kernel(
    nr, ng, wire,
    perturb, start_block, eofs, loadings_t,
    proj, gram, gpair, gchunk, gfull, panel, ppair, pchunk, pfull, basis, work, inverse,
    s_g0, r_g0, s_g1, r_g1, s_g2, r_g2, s_p0, r_p0, s_p1, r_p1, s_p2, r_p2, s_p3, r_p3, s_p4, r_p4,
):
    r, g = lax.axis_index("rows"), lax.axis_index("grp")
    rows, columns = perturb.shape
    rank = start_block.shape[1]
    padded = panel.shape[2]
    part = rank // ng
    piece = gchunk.shape[2]
    row_tile = math.gcd(rows, 256)

    def row_peer(o):
        return lax.rem(r + o, nr)

    def grp_peer(o):
        return lax.rem(g + o, ng)

    barrier = pltpu.get_barrier_semaphore()

    def greet_row(o):
        pl.semaphore_signal(barrier, inc=1, device_id=(row_peer(o), g), device_id_type=MESH)

    def greet_grp(o):
        pl.semaphore_signal(barrier, inc=1, device_id=(r, grp_peer(o)), device_id_type=MESH)

    each(1, nr, greet_row)
    each(1, ng, greet_grp)

    def remote(src, dst, send, recv, device):
        return pltpu.make_async_remote_copy(
            src_ref=src, dst_ref=dst, send_sem=send, recv_sem=recv,
            device_id=device, device_id_type=MESH,
        )

    own_rank = pl.ds(pl.multiple_of(g * part, part), part)
    own_columns = pl.ds(pl.multiple_of(r * LANES, LANES), LANES)

    def lanes_of(index):
        return pl.ds(pl.multiple_of(index * LANES, LANES), LANES)

    def pieces_of(index):
        return pl.ds(pl.multiple_of(index * piece, piece), piece)

    for it in range(ITERS):
        for at in range(0, rows, row_tile):
            tile = perturb[at : at + row_tile, :]
            if it == 0:
                product = jnp.dot(tile, start_block[...], preferred_element_type=F32)
            else:
                product = nt_dot(tile, basis[it - 1, :, :columns])
            proj[at : at + row_tile, :] = product.astype(BF16)
        proj_t = proj[...].T
        gpair[it, g] = nt_dot(proj_t, proj_t)
        if it == 0:
            pl.semaphore_wait(barrier, nr - 1 + ng - 1)

        def g0(o):
            return remote(gpair.at[it, g], gpair.at[it, g], s_g0.at[it, o], r_g0.at[it, o], (r, grp_peer(o)))

        def g1(o):
            return remote(
                gram.at[it, pieces_of(row_peer(o))], gchunk.at[it, r],
                s_g1.at[it, o], r_g1.at[it, o], (row_peer(o), g),
            )

        def g2(o):
            return remote(
                gfull.at[it, pieces_of(r)], gfull.at[it, pieces_of(r)],
                s_g2.at[it, o], r_g2.at[it, o], (row_peer(o), g),
            )

        def p0(o):
            there = pl.ds(pl.multiple_of(grp_peer(o) * part, part), part)
            return remote(panel.at[it, there], ppair.at[it, g], s_p0.at[it, o], r_p0.at[it, o], (r, grp_peer(o)))

        def p1(o):
            return remote(
                ppair.at[it, g, :, lanes_of(row_peer(o))], pchunk.at[it, r],
                s_p1.at[it, o], r_p1.at[it, o], (row_peer(o), g),
            )

        def p2(o):
            return remote(pfull.at[it, own_rank], pfull.at[it, own_rank], s_p2.at[it, o], r_p2.at[it, o], (r, grp_peer(o)))

        def p3(o):
            block = basis.at[it, own_rank, own_columns]
            return remote(block, block, s_p3.at[it, o], r_p3.at[it, o], (row_peer(o), g))

        def p4(o, q):
            block = basis.at[it, own_rank, lanes_of(lax.rem(r + nr - o, nr))]
            return remote(block, block, s_p4.at[it, o, q], r_p4.at[it, o, q], (r, grp_peer(q)))

        each(1, ng, lambda o: g0(o).start())
        steps = [(at, min(at + 512, columns)) for at in range(0, columns, 512)]

        def panel_steps(chosen):
            for at, to in chosen:
                panel[it, :, at:to] = jnp.dot(proj_t, perturb[:, at:to], preferred_element_type=F32)

        if padded > columns:
            floor = columns // LANES * LANES
            panel[it, :, floor:] = jnp.zeros((rank, padded - floor), F32)
        panel_steps(steps[:1])
        each(1, ng, lambda o: g0(o).wait())
        total = gpair[it, 0]
        for index in range(1, ng):
            total = total + gpair[it, index]
        gram[it, :rank] = total
        each(1, nr, lambda o: g1(o).start())
        gchunk[it, r] = gram[it, pieces_of(r)]
        panel_steps(steps[1:])
        each(1, ng, lambda o: p0(o).start())
        ppair[it, g] = panel[it, own_rank]
        each(1, nr, lambda o: g1(o).wait())
        gfull[it, pieces_of(r)] = jnp.sum(gchunk[it], axis=0)
        each(1, nr, lambda o: g2(o).start())
        each(1, ng, lambda o: p0(o).wait())
        total = ppair[it, 0]
        for index in range(1, ng):
            total = total + ppair[it, index]
        ppair[it, g] = total
        each(1, nr, lambda o: g2(o).wait())
        each(1, nr, lambda o: p1(o).start())
        pchunk[it, r] = ppair[it, g, :, own_columns]
        work[:, :rank] = gfull[it, :rank]
        inverse_factor(work, inverse)
        each(1, nr, lambda o: p1(o).wait())
        pfull[it, own_rank] = jnp.sum(pchunk[it], axis=0)
        each(1, ng, lambda o: p2(o).start())
        each(1, ng, lambda o: p2(o).wait())
        weights = jnp.dot(
            inverse[own_rank, :], pfull[it], precision=lax.Precision.HIGHEST, preferred_element_type=F32
        )
        basis[it, own_rank, own_columns] = weights.astype(BF16)
        each(1, nr, lambda o: p3(o).start())
        each(1, ng, lambda q: p4(0, q).start())
        if it == ITERS - 1:
            for at in range(0, rows, row_tile):
                eofs[at : at + row_tile, :] = nt_dot(
                    proj[at : at + row_tile, :].astype(F32), inverse[...], precision=lax.Precision.HIGHEST
                )

        def forward(o):
            p3(o).wait()
            each(1, ng, lambda q: p4(o, q).start())

        each(1, nr, forward)
        each(0, nr, lambda o: each(1, ng, lambda q: p4(o, q).wait()))
    loadings_t[...] = basis[ITERS - 1, :, :columns]


def on_device(perturb, start_block, *, nr, ng):
    rows, columns = perturb.shape
    rank = start_block.shape[1]
    total_rows = rows * nr * ng
    slab = columns // ng
    padded = max(LANES * nr, round_up(columns, LANES))
    piece = round_up(-(-rank // nr), 8)
    part = rank // ng
    dma = pltpu.SemaphoreType.DMA
    sems = []
    for n in (ng, nr, nr, ng, nr, ng, nr):
        sems += [dma((ITERS, n))] * 2
    sems += [dma((ITERS, nr, ng))] * 2
    vmem = pl.BlockSpec(memory_space=pltpu.VMEM)
    eofs, loadings_t = pl.pallas_call(
        functools.partial(kernel, nr, ng, F32),
        out_shape=(
            jax.ShapeDtypeStruct((rows, rank), F32),
            jax.ShapeDtypeStruct((rank, columns), BF16),
        ),
        in_specs=[vmem, vmem],
        out_specs=(vmem, vmem),
        scratch_shapes=[
            pltpu.VMEM((rows, rank), BF16),
            pltpu.VMEM((ITERS, piece * nr, rank), F32),
            pltpu.VMEM((ITERS, ng, rank, rank), F32),
            pltpu.VMEM((ITERS, nr, piece, rank), F32),
            pltpu.VMEM((ITERS, piece * nr, rank), F32),
            pltpu.VMEM((ITERS, rank, padded), F32),
            pltpu.VMEM((ITERS, ng, part, padded), F32),
            pltpu.VMEM((ITERS, nr, part, LANES), F32),
            pltpu.VMEM((ITERS, rank, LANES), F32),
            pltpu.VMEM((ITERS, rank, padded), BF16),
            pltpu.VMEM((rank, 2 * rank), F32),
            pltpu.VMEM((rank, rank), F32),
        ] + sems,
        compiler_params=pltpu.CompilerParams(
            collective_id=0, has_side_effects=True, vmem_limit_bytes=60 * 1024 * 1024
        ),
    )(perturb, start_block)
    own = lax.dynamic_slice_in_dim(loadings_t, lax.axis_index("grp") * slab, slab, 1).astype(F32).T
    return eofs * math.sqrt(total_rows), own * math.sqrt(columns / total_rows)


def solution(mesh):
    return jax.shard_map(
        functools.partial(on_device, nr=mesh.shape["rows"], ng=mesh.shape["grp"]),
        mesh=mesh,
        in_specs=(P(("rows", "grp"), None), P()),
        out_specs=(P(("rows", "grp"), None), P("grp", None)),
        check_vma=False,
    )
```
